256 devices in a mesh: wide: 64 (over z, y, core), narrow: 4 (over x).
Axes of the slice: x: 4, y: 4, z: 8, core: 2. Of those that a mesh axis runs over, the one named last changes fastest.
Arguments:
- coords_inner: float32 [2, 65536], P(None, ('wide', 'narrow')), may hold values from -1 to 1
- velocity: float32 [2, 65536], P(None, ('wide', 'narrow')), may hold values from -6 to 6
- source: float32 [65536], P(('wide', 'narrow')), may hold values from -6 to 6
- coords_edge: float32 [2, 32768], P(None, ('wide', 'narrow')), may hold values from -1 to 1
- flux_weight: float32 [2, 32768], P(None, ('wide', 'narrow')), may hold values from -6 to 6
- owner: int32 [32768, 1], P(('wide', 'narrow')), may hold values from 0 to 63; in each aligned block of 128 rows (0 to 127, 128 to 255, ...) at most 4 rows name the same one
- local_face: int32 [32768], P(('wide', 'narrow')), may hold values from 0 to 127
- w_first: float32 [2, 512], replicated, may hold values from -4 to 4
- b_first: float32 [512], replicated, may hold values from -3 to 3
- w_hidden: float32 [4, 512, 512], replicated, may hold values from -0.25 to 0.25
- b_hidden: float32 [4, 512], replicated, may hold values from -3 to 3
- w_last: float32 [512], replicated, may hold values from -0.25 to 0.25
Outputs:
- face_integral: float32 [8192], P('wide')
- grad_first: float32 [2, 512], replicated
- grad_hidden: float32 [4, 512, 512], replicated
- grad_last: float32 [512], replicated
The draws below stay inside these ranges and needn't reach their ends.
Inputs may be any that keep to these rules, and one draw needn't show every extreme that they name: Among the 128 face points of one device no owner appears more than 4 times, and some owner appears exactly 4 times.
All inputs are finite; a program needn't handle non-finite values.
Results may differ from the reference program's by a relative error of at most 0.0003.
Values sent between devices are 32-bit elements; how exact they have to be, the bound alone decides.
A program may use at most 128 MiB of HBM per device.

```python
import math
import jax
import jax.numpy as jnp
import numpy as np
from jax import lax

D = 512
LAYERS = 4
PB = 128
FACE_DEV = 128
CAP = 4
NPI = 65536
NPB = 32768
NF = 8192
N_WIDE = 64
N_NARROW = 4


def draw_w_first(key, part):
    values = jax.random.uniform(jax.random.fold_in(key, 13), (2, D), jnp.float32, -4.0, 4.0)
    return values.astype(jnp.float32)


def draw_w_hidden(key, part):
    values = jnp.clip(0.15 * jax.random.normal(jax.random.fold_in(key, 22), (LAYERS, D, D), jnp.float32), -0.25, 0.25)
    return values.astype(jnp.float32)


def touch_ends(drawn, rng, smallest, high):
    longest = drawn.shape.index(max(drawn.shape))
    spots = []
    for shift in (0, 1):
        where = [jax.random.randint(jax.random.fold_in(rng, axis), (), 0, length) for axis, length in enumerate(drawn.shape)]
        where[longest] = (where[longest] + shift) % drawn.shape[longest]
        spots.append(tuple(where))
    return drawn.at[spots[0]].set(smallest).at[spots[1]].set(high)


def steps_of(rng, dims, shards, low, top_value):
    level = 1.0
    for dim, shards_of in shards:
        steps = jax.random.uniform(jax.random.fold_in(jax.random.fold_in(rng, 6), dim), (shards_of,), jnp.float32, low / len(shards), top_value / len(shards))
        level = level * jnp.repeat(jnp.exp(steps), dims[dim] // shards_of).reshape((-1,) + (1,) * (len(dims) - 1 - dim))
    return level


def assign_block(own_key, own, number, rows, number_of, top, reach, skew):
    ranking = jax.random.permutation(own_key, number_of)
    packed, common = load_shares(number_of, rows * top, reach, skew, True), load_shares(number_of, rows * top, reach, skew, False)
    places = jnp.arange(number_of)

    def named(tallies, offset_by):
        used = int((tallies > 0).sum())
        fixed = max(1, used // 4)
        passed = fixed + (places - fixed + offset_by * (used - fixed)) % max(1, number_of - fixed)
        return jnp.zeros((number_of,), jnp.int32).at[ranking[jnp.where(places < fixed, places, passed)]].set(jnp.asarray(tallies, jnp.int32))

    tallies = jnp.where(number % 4 == 0, named(packed, number // 4), named(common, number - number // 4 - 1))
    mixed = jax.random.permutation(jax.random.fold_in(own, 3), number_of)
    source_of, receiver = mixed[0:number_of // 2 * 2:2], mixed[1:number_of // 2 * 2:2]
    margin = jnp.minimum(tallies[source_of] - 1, reach - tallies[receiver]) // 2
    margin = jnp.where((source_of == ranking[0]) | (receiver == ranking[0]) | (tallies[receiver] == 0), 0, jnp.maximum(margin, 0))
    passed = jax.random.randint(jax.random.fold_in(own, 4), (number_of // 2,), 0, 1 << 20) % (margin + 1)
    tallies = tallies.at[source_of].add(-passed).at[receiver].add(passed)
    labels = jnp.searchsorted(jnp.cumsum(tallies), jnp.arange(rows * top), side="right").astype(jnp.int32)
    listing = labels.reshape(top, rows).T
    listing = listing[jax.random.permutation(jax.random.fold_in(own, 1), rows)]
    offset_by = jax.random.randint(jax.random.fold_in(own, 2), (rows, 1), 0, top)
    return jnp.take_along_axis(listing, (jnp.arange(top)[None, :] + offset_by) % top, axis=1)


def load_shares(count, total, limit, skew, full):
    loads = [(1 << 20) // math.isqrt(standing ** skew) + 1 for standing in range(1, count + 1)]
    largest = limit if full else min(limit, max(-(-total // count), total * loads[0] // sum(loads)))
    least = 1 if total - largest >= count - 1 else 0
    given, surplus = [largest] + [least] * (count - 1), total - largest - least * (count - 1)
    while surplus > 0:
        candidates = [i for i in range(1, count) if given[i] < largest] or [i for i in range(1, count) if given[i] < limit]
        mass, left = sum([loads[i] for i in candidates]), surplus
        for i in candidates:
            more = min(limit - given[i], max(1, left * loads[i] // mass), surplus)
            given[i] = given[i] + more
            surplus = surplus - more
    return np.array(given)


def scatter_about(stream_key, extent, scale, most, cuts=(), held_as=jnp.bfloat16):
    entries = jax.random.normal(stream_key, extent, jnp.float32) * scale
    if len(cuts) > 0:
        entries = steps_of(stream_key, extent, cuts, -0.22, 0.18) * entries
    return jnp.clip(entries, min=-most, max=most).astype(held_as)


def setup_inputs(seed: int = 0) -> dict:
    key_of = jax.random.split(jax.random.key(seed), 13)
    coords_inner = jnp.clip(jax.random.uniform(key_of[0], (2, NPI), jnp.float32, -1.0, 1.0) * steps_of(key_of[0], (2, NPI), ((1, 256),), -0.4, 0.0), -1.0, 1.0)
    velocity = scatter_about(key_of[1], (2, NPI), 1.0, 6.0, ((1, 256),), jnp.float32)
    source = scatter_about(key_of[2], (NPI,), 1.0, 6.0, ((0, 256),), jnp.float32)
    coords_edge = jnp.clip(jax.random.uniform(key_of[3], (2, NPB), jnp.float32, -1.0, 1.0) * steps_of(key_of[3], (2, NPB), ((1, 256),), -0.4, 0.0), -1.0, 1.0)
    flux_weight = scatter_about(key_of[4], (2, NPB), 1.0, 6.0, ((1, 256),), jnp.float32)
    owner_keys = jax.random.split(jax.random.fold_in(key_of[5], 1), NPB // PB)
    owner_turns = jax.random.permutation(jax.random.fold_in(key_of[5], 3), NPB // PB)
    owner = jax.vmap(lambda own, number: assign_block(jax.random.fold_in(key_of[5], 2), own, number, PB, N_WIDE, 1, CAP, 2))(owner_keys, owner_turns).reshape((NPB, 1))
    local_face = touch_ends(jax.random.randint(key_of[6], (NPB,), 0, FACE_DEV), jax.random.fold_in(key_of[6], 1), 0, FACE_DEV - 1).astype(jnp.int32)
    w_first = draw_w_first(jax.random.fold_in(key_of[12], 71), 0)
    b_first = scatter_about(key_of[8], (D,), 0.5, 3.0, (), jnp.float32)
    w_hidden = draw_w_hidden(jax.random.fold_in(key_of[12], 71), 0)
    b_hidden = scatter_about(key_of[10], (LAYERS, D), 0.5, 3.0, (), jnp.float32)
    w_last = scatter_about(key_of[11], (D,), D ** -0.5, 0.25, (), jnp.float32)
    return {"coords_inner": coords_inner, "velocity": velocity, "source": source, "coords_edge": coords_edge, "flux_weight": flux_weight, "owner": owner, "local_face": local_face, "w_first": w_first, "b_first": b_first, "w_hidden": w_hidden, "b_hidden": b_hidden, "w_last": w_last}


precise = lax.Precision.HIGHEST
penalty_weight = 4.0

def network(weights, biases, coords):
    w_first, w_hidden, w_last = weights
    b_first, b_hidden = biases
    point_count = coords.shape[1]
    feature_width = w_first.shape[1]
    hidden = jnp.tanh(jnp.dot(coords.T, w_first, precision=precise) + b_first)
    tangent = (1.0 - hidden * hidden)[None] * w_first[:, None, :]
    for level_index in range(w_hidden.shape[0]):
        stacked = jnp.concatenate([hidden[None], tangent], 0).reshape(3 * point_count, feature_width)
        product = jnp.dot(stacked, w_hidden[level_index], precision=precise)
        hidden = jnp.tanh(product[:point_count] + b_hidden[level_index])
        tangent = (1.0 - hidden * hidden)[None] * product[point_count:].reshape(2, point_count, feature_width)
    point_value = jnp.dot(hidden, w_last, precision=precise)
    slopes = jnp.dot(tangent.reshape(2 * point_count, feature_width), w_last, precision=precise).reshape(2, point_count)
    return (point_value, slopes)

def residual(weights, biases, coords, velocity, source):
    point_value, slopes = network(weights, biases, coords)
    return velocity[0] * slopes[0] + velocity[1] * slopes[1] + point_value - source

def edge_flux(weights, biases, coords, flux_weight):
    _, slopes = network(weights, biases, coords)
    return flux_weight[0] * slopes[0] + flux_weight[1] * slopes[1]

def reference(coords_inner, velocity, source, coords_edge, flux_weight, owner, local_face, w_first, b_first, w_hidden, b_hidden, w_last):
    weights = (w_first, w_hidden, w_last)
    biases = (b_first, b_hidden)
    blocks = N_WIDE * N_NARROW

    def split(array):
        shaped = array.reshape(array.shape[:-1] + (blocks, array.shape[-1] // blocks))
        return jnp.moveaxis(shaped, -2, 0)
    edge_coords = split(coords_edge)
    edge_weight = split(flux_weight)
    fluxes = lax.map(lambda pair: edge_flux(weights, biases, pair[0], pair[1]), (edge_coords, edge_weight)).reshape(-1)
    face_index = owner[:, 0] * FACE_DEV + local_face
    integral = jax.ops.segment_sum(fluxes, face_index, num_segments=NF)
    edge_cot = split(2.0 * penalty_weight / math.sqrt(NF) * integral[face_index])

    def accumulate(totals, pieces):
        inner_c, inner_v, inner_s, edge_c, edge_w, cotangent = pieces
        residuals, inner_pull = jax.vjp(lambda params: residual(params, biases, inner_c, inner_v, inner_s), weights)
        inner_grads = inner_pull(2.0 / math.sqrt(NPI) * residuals)[0]
        _, edge_pull = jax.vjp(lambda params: edge_flux(params, biases, edge_c, edge_w), weights)
        edge_grads = edge_pull(cotangent)[0]
        return (jax.tree.map(lambda first, second, third: first + second + third, totals, inner_grads, edge_grads), None)
    start = (jnp.zeros_like(w_first), jnp.zeros_like(w_hidden), jnp.zeros_like(w_last))
    totals, _ = lax.scan(accumulate, start, (split(coords_inner), split(velocity), split(source), edge_coords, edge_weight, edge_cot))
    return (integral, totals[0], totals[1], totals[2])
```

```python
import math

import jax
import jax.numpy as jnp
from jax import lax
from jax.sharding import PartitionSpec as P

FACE_DEV = 128
penalty_weight = 4.0
BOTH = ("wide", "narrow")
precise = lax.Precision.HIGH


def forward(coords, direction, w_first, b_first, w_hidden, b_hidden, w_last):
    hidden = jnp.tanh(
        coords[0][:, None] * w_first[0][None] + coords[1][:, None] * w_first[1][None] + b_first
    )
    tangent = (1.0 - hidden * hidden) * (
        direction[0][:, None] * w_first[0][None] + direction[1][:, None] * w_first[1][None]
    )
    points = hidden.shape[0]
    kept = [(hidden, None, tangent)]
    for level in range(w_hidden.shape[0]):
        product = jnp.dot(
            jnp.concatenate([hidden, tangent], 0), w_hidden[level], precision=precise
        )
        hidden = jnp.tanh(product[:points] + b_hidden[level])
        slope = product[points:]
        tangent = (1.0 - hidden * hidden) * slope
        kept.append((hidden, slope, tangent))
    value = jnp.sum(hidden * w_last[None], 1)
    slopes = jnp.sum(tangent * w_last[None], 1)
    return value, slopes, kept


def backward(coords, direction, kept, hidden_cot, tangent_cot, w_first, w_hidden):
    grads = []
    for level in reversed(range(w_hidden.shape[0])):
        hidden, slope, _ = kept[level + 1]
        gate = 1.0 - hidden * hidden
        product_cot = gate * tangent_cot
        sum_cot = gate * (hidden_cot - 2.0 * hidden * slope * tangent_cot)
        cots = jnp.concatenate([sum_cot, product_cot], 0)
        below = jnp.concatenate([kept[level][0], kept[level][2]], 0)
        grads.append(
            lax.dot_general(below, cots, (((0,), (0,)), ((), ())), precision=precise)
        )
        down = lax.dot_general(cots, w_hidden[level], (((1,), (1,)), ((), ())), precision=precise)
        points = hidden.shape[0]
        hidden_cot, tangent_cot = down[:points], down[points:]
    hidden, _, _ = kept[0]
    gate = 1.0 - hidden * hidden
    start = direction[0][:, None] * w_first[0][None] + direction[1][:, None] * w_first[1][None]
    start_cot = gate * tangent_cot
    sum_cot = gate * (hidden_cot - 2.0 * hidden * start * tangent_cot)
    first = jnp.stack(
        [
            jnp.sum(coords[j][:, None] * sum_cot + direction[j][:, None] * start_cot, 0)
            for j in range(2)
        ]
    )
    return first, jnp.stack(grads[::-1], 0)


def local(
    coords_inner,
    velocity,
    source,
    coords_edge,
    flux_weight,
    owner,
    local_face,
    w_first,
    b_first,
    w_hidden,
    b_hidden,
    w_last,
):
    devices = lax.axis_size(BOTH)
    inner_rows = coords_inner.shape[1]
    edge_rows = coords_edge.shape[1]
    inner_scale = 2.0 / math.sqrt(inner_rows * devices)
    face_scale = 2.0 * penalty_weight / math.sqrt(FACE_DEV * lax.axis_size("wide"))
    net = (w_first, b_first, w_hidden, b_hidden, w_last)

    _, flux, kept_edge = forward(coords_edge, flux_weight, *net)
    face = owner[:, 0] * FACE_DEV + local_face
    mine = jnp.stack([flux, face.astype(jnp.float32)], 0)
    everyone = lax.all_gather(mine, BOTH)
    all_flux = everyone[:, 0].reshape(-1)
    all_face = everyone[:, 1].reshape(-1)

    def sums(wanted):
        return jnp.sum(
            jnp.where(wanted.astype(jnp.float32)[:, None] == all_face[None], all_flux[None], 0.0), 1
        )

    reached = sums(face)
    integral = sums(lax.axis_index("wide") * FACE_DEV + jnp.arange(FACE_DEV))

    value, slopes, kept_inner = forward(coords_inner, velocity, *net)
    inner_cot = inner_scale * (slopes + value - source)
    edge_cot = face_scale * reached

    coords = jnp.concatenate([coords_inner, coords_edge], 1)
    direction = jnp.concatenate([velocity, flux_weight], 1)
    kept = [
        tuple(None if a is None else jnp.concatenate([a, b], 0) for a, b in zip(one, two))
        for one, two in zip(kept_inner, kept_edge)
    ]
    hidden_out = jnp.concatenate([inner_cot, jnp.zeros_like(edge_cot)])[:, None]
    tangent_out = jnp.concatenate([inner_cot, edge_cot])[:, None]
    last = jnp.sum(hidden_out * kept[-1][0] + tangent_out * kept[-1][2], 0)
    first, hidden = backward(
        coords,
        direction,
        kept,
        hidden_out * w_last[None],
        tangent_out * w_last[None],
        w_first,
        w_hidden,
    )
    first, hidden, last = lax.psum((first, hidden, last), BOTH)
    return integral, first, hidden, last


def solution(mesh):
    points = P(None, BOTH)
    in_specs = (
        points,
        points,
        P(BOTH),
        points,
        points,
        P(BOTH, None),
        P(BOTH),
        P(),
        P(),
        P(),
        P(),
        P(),
    )
    out_specs = (P("wide"), P(), P(), P())
    return jax.shard_map(local, mesh=mesh, in_specs=in_specs, out_specs=out_specs, check_vma=False)
```

```python
import math

import jax
import jax.numpy as jnp
from jax import lax
from jax.experimental import pallas as pl
from jax.experimental.pallas import tpu as pltpu
from jax.sharding import PartitionSpec as P

MESH = pl.DeviceIdType.MESH

FACE_DEV = 128
penalty_weight = 4.0
BOTH = ("wide", "narrow")
precise = lax.Precision.HIGH
FACES = 64
CHUNKS = 4
TILES = 256


def place():
    wide = lax.axis_index("wide")
    x = lax.axis_index("narrow")
    return x, (wide // 2) % 4, wide // 8, wide % 2


def device(x, y, z, core):
    return {"wide": (z * 4 + y) * 2 + core, "narrow": x}


def peers_x(d):
    x, y, z, core = place()
    return device((x + d) % 4, y, z, core)


def peers_y(d):
    x, y, z, core = place()
    return device(x, (y + d) % 4, z, core)


def peers_z(d):
    x, y, z, core = place()
    return device(x, y, (z + d) % 8, core)


def partner():
    x, y, z, core = place()
    return device(x, y, z, 1 - core)


def along_first(d):
    x, y, z, core = place()
    return device((x + d * (1 - core)) % 4, (y + d * core) % 4, z, core)


def along_second(d):
    x, y, z, core = place()
    return device((x + d * core) % 4, (y + d * (1 - core)) % 4, z, core)


def greet():
    barrier = pltpu.get_barrier_semaphore()
    others = (
        [partner()]
        + [peers_x(d) for d in range(1, 4)]
        + [peers_y(d) for d in range(1, 4)]
        + [peers_z(d) for d in range(1, 8)]
    )
    for other in others:
        pl.semaphore_signal(barrier, inc=1, device_id=other, device_id_type=MESH)
    pl.semaphore_wait(barrier, len(others))


def remote(src, dst, sems, index, target):
    return pltpu.make_async_remote_copy(
        src_ref=src,
        dst_ref=dst,
        send_sem=sems[0].at[index],
        recv_sem=sems[1].at[index],
        device_id=target,
        device_id_type=MESH,
    )


def faces_kernel(mine_ref, all_ref, row, got, send, recv):
    x, y, z, core = place()
    sems = (send, recv)
    greet()
    spot = lax.broadcasted_iota(jnp.int32, (8, 128), 0)
    row[...] = jnp.where(spot == x, mine_ref[0:1, :], 0.0) + jnp.where(
        spot == x + 4, mine_ref[1:2, :], 0.0
    )
    copies = [remote(row, got.at[d - 1], sems, d - 1, peers_x(d)) for d in range(1, 4)]
    for copy in copies:
        copy.start()
    for copy in copies:
        copy.wait()
    at = core * 32 + z * 4
    all_ref[at + y] = row[...] + got[0] + got[1] + got[2]
    here = all_ref.at[at + y]
    copies = [remote(here, here, sems, 2 + d, peers_y(d)) for d in range(1, 4)]
    for copy in copies:
        copy.start()
    for copy in copies:
        copy.wait()
    here = all_ref.at[pl.ds(at, 4)]
    copies = [remote(here, here, sems, 5 + d, peers_z(d)) for d in range(1, 8)]
    for copy in copies:
        copy.start()
    for copy in copies:
        copy.wait()
    here = all_ref.at[pl.ds(core * 32, 32)]
    copy = remote(here, here, sems, 13, partner())
    copy.start()
    copy.wait()


def gather_faces(flux, face):
    mine = jnp.stack([flux, face.astype(jnp.float32)], 0)
    return pl.pallas_call(
        faces_kernel,
        out_shape=jax.ShapeDtypeStruct((FACES, 8, 128), jnp.float32),
        in_specs=[pl.BlockSpec(memory_space=pltpu.VMEM)],
        out_specs=pl.BlockSpec(memory_space=pltpu.VMEM),
        scratch_shapes=[
            pltpu.VMEM((8, 128), jnp.float32),
            pltpu.VMEM((3, 8, 128), jnp.float32),
            pltpu.SemaphoreType.DMA((14,)),
            pltpu.SemaphoreType.DMA((14,)),
        ],
        compiler_params=pltpu.CompilerParams(collective_id=0, has_side_effects=True),
    )(mine)


def reduce_steps(k, grad, total, bufs, sems):
    core_in, first_in, second_in, third_in, half, quarter, piece = bufs
    x, y, z, core = place()
    p1 = x * (1 - core) + y * core
    p2 = y * (1 - core) + x * core
    half_at = core * 128
    first_at = half_at + p1 * 32
    second_at = first_at + p2 * 8
    base = k * 28
    copies = {}

    def launch(name, made):
        copies[name] = made
        for copy in made:
            copy.start()

    def settle(name):
        for copy in copies[name]:
            copy.wait()

    def s0():
        src = grad.at[k, pl.ds((1 - core) * 128, 128)]
        launch("core", [remote(src, core_in.at[k], sems, base, partner())])

    def s1():
        settle("core")
        half[k] = grad[k, pl.ds(half_at, 128)] + core_in[k]
        launch(
            "first",
            [
                remote(
                    half.at[k, pl.ds(((p1 + d) % 4) * 32, 32)],
                    first_in.at[k, d - 1],
                    sems,
                    base + d,
                    along_first(d),
                )
                for d in range(1, 4)
            ],
        )

    def s2():
        settle("first")
        quarter[k] = (half[k, pl.ds(p1 * 32, 32)] + first_in[k, 0]) + (
            first_in[k, 1] + first_in[k, 2]
        )
        launch(
            "second",
            [
                remote(
                    quarter.at[k, pl.ds(((p2 + d) % 4) * 8, 8)],
                    second_in.at[k, d - 1],
                    sems,
                    base + 3 + d,
                    along_second(d),
                )
                for d in range(1, 4)
            ],
        )

    def s3():
        settle("second")
        piece[k] = (quarter[k, pl.ds(p2 * 8, 8)] + second_in[k, 0]) + (
            second_in[k, 1] + second_in[k, 2]
        )
        launch(
            "third",
            [
                remote(piece.at[k, (z + d) % 8], third_in.at[k, d - 1], sems, base + 6 + d, peers_z(d))
                for d in range(1, 8)
            ],
        )

    def s4():
        settle("third")
        done = piece[k, z]
        for d in range(7):
            done = done + third_in[k, d]
        total[k, second_at + z] = done
        here = total.at[k, second_at + z]
        launch("z", [remote(here, here, sems, base + 13 + d, peers_z(d)) for d in range(1, 8)])

    def s5():
        settle("z")
        here = total.at[k, pl.ds(second_at, 8)]
        launch("b", [remote(here, here, sems, base + 20 + d, along_second(d)) for d in range(1, 4)])

    def s6():
        settle("b")
        here = total.at[k, pl.ds(first_at, 32)]
        launch("a", [remote(here, here, sems, base + 23 + d, along_first(d)) for d in range(1, 4)])

    def s7():
        settle("a")
        here = total.at[k, pl.ds(half_at, 128)]
        launch("end", [remote(here, here, sems, base + 27, partner())])

    def s8():
        settle("end")

    return [s0, s1, s2, s3, s4, s5, s6, s7, s8]


def small_steps(small, small_out, got, part, sems, base):
    x, y, z, core = place()
    copies = {}

    def launch(name, src, at, count, peer):
        copies[name] = [
            remote(src, got.at[at + d - 1], sems, base + at + d - 1, peer(d)) for d in range(1, count)
        ]
        for copy in copies[name]:
            copy.start()

    def ordered(mine, at, count, place_of):
        result = None
        for member in range(count):
            value = jnp.where(place_of == member, mine, 0.0)
            for d in range(1, count):
                value = value + jnp.where((place_of - d) % count == member, got[at + d - 1], 0.0)
            result = value if result is None else result + value
        return result

    def s0():
        launch("core", small, 0, 2, lambda d: partner())

    def s1():
        copies["core"][0].wait()
        part[0] = ordered(small[...], 0, 2, core)
        launch("x", part.at[0], 1, 4, peers_x)

    def s2():
        for copy in copies["x"]:
            copy.wait()
        part[1] = ordered(part[0], 1, 4, x)
        launch("y", part.at[1], 4, 4, peers_y)

    def s3():
        for copy in copies["y"]:
            copy.wait()
        part[2] = ordered(part[1], 4, 4, y)
        launch("z", part.at[2], 7, 8, peers_z)

    def s4():
        for copy in copies["z"]:
            copy.wait()
        small_out[...] = ordered(part[2], 7, 8, z)

    return [s0, s1, s2, s3, s4]


def sum_kernel(
    grad,
    small,
    total,
    small_out,
    core_in,
    first_in,
    second_in,
    third_in,
    half,
    quarter,
    piece,
    small_in,
    small_part,
    send,
    recv,
):
    sems = (send, recv)
    greet()
    bufs = (core_in, first_in, second_in, third_in, half, quarter, piece)
    chunks = [reduce_steps(k, grad, total, bufs, sems) for k in range(CHUNKS)]
    chunks.append(small_steps(small, small_out, small_in, small_part, sems, CHUNKS * 28))
    for turn in range(CHUNKS + 9):
        for k, steps in enumerate(chunks):
            if 0 <= turn - k < len(steps):
                steps[turn - k]()


def sum_grads(grad, small):
    tile = (8, 128)
    count = CHUNKS * 28 + 14
    return pl.pallas_call(
        sum_kernel,
        out_shape=(
            jax.ShapeDtypeStruct((CHUNKS, TILES) + tile, jnp.float32),
            jax.ShapeDtypeStruct((2,) + tile, jnp.float32),
        ),
        in_specs=[pl.BlockSpec(memory_space=pltpu.VMEM)] * 2,
        out_specs=(pl.BlockSpec(memory_space=pltpu.VMEM),) * 2,
        scratch_shapes=[
            pltpu.VMEM((CHUNKS, 128) + tile, jnp.float32),
            pltpu.VMEM((CHUNKS, 3, 32) + tile, jnp.float32),
            pltpu.VMEM((CHUNKS, 3, 8) + tile, jnp.float32),
            pltpu.VMEM((CHUNKS, 7) + tile, jnp.float32),
            pltpu.VMEM((CHUNKS, 128) + tile, jnp.float32),
            pltpu.VMEM((CHUNKS, 32) + tile, jnp.float32),
            pltpu.VMEM((CHUNKS, 8) + tile, jnp.float32),
            pltpu.VMEM((14, 2) + tile, jnp.float32),
            pltpu.VMEM((3, 2) + tile, jnp.float32),
            pltpu.SemaphoreType.DMA((count,)),
            pltpu.SemaphoreType.DMA((count,)),
        ],
        compiler_params=pltpu.CompilerParams(
            collective_id=1, has_side_effects=True, vmem_limit_bytes=40 * 2**20
        ),
    )(grad, small)


def forward(coords, direction, w_first, b_first, w_hidden, b_hidden, w_last):
    hidden = jnp.tanh(
        coords[0][:, None] * w_first[0][None] + coords[1][:, None] * w_first[1][None] + b_first
    )
    tangent = (1.0 - hidden * hidden) * (
        direction[0][:, None] * w_first[0][None] + direction[1][:, None] * w_first[1][None]
    )
    points = hidden.shape[0]
    kept = [(hidden, None, tangent)]
    for level in range(w_hidden.shape[0]):
        product = jnp.dot(
            jnp.concatenate([hidden, tangent], 0), w_hidden[level], precision=precise
        )
        hidden = jnp.tanh(product[:points] + b_hidden[level])
        slope = product[points:]
        tangent = (1.0 - hidden * hidden) * slope
        kept.append((hidden, slope, tangent))
    value = jnp.sum(hidden * w_last[None], 1)
    slopes = jnp.sum(tangent * w_last[None], 1)
    return value, slopes, kept


def backward(coords, direction, kept, hidden_cot, tangent_cot, w_first, w_hidden):
    grads = []
    for level in reversed(range(w_hidden.shape[0])):
        hidden, slope, _ = kept[level + 1]
        gate = 1.0 - hidden * hidden
        product_cot = gate * tangent_cot
        sum_cot = gate * (hidden_cot - 2.0 * hidden * slope * tangent_cot)
        cots = jnp.concatenate([sum_cot, product_cot], 0)
        below = jnp.concatenate([kept[level][0], kept[level][2]], 0)
        grads.append(
            lax.dot_general(below, cots, (((0,), (0,)), ((), ())), precision=precise)
        )
        down = lax.dot_general(cots, w_hidden[level], (((1,), (1,)), ((), ())), precision=precise)
        points = hidden.shape[0]
        hidden_cot, tangent_cot = down[:points], down[points:]
    hidden, _, _ = kept[0]
    gate = 1.0 - hidden * hidden
    start = direction[0][:, None] * w_first[0][None] + direction[1][:, None] * w_first[1][None]
    start_cot = gate * tangent_cot
    sum_cot = gate * (hidden_cot - 2.0 * hidden * start * tangent_cot)
    first = jnp.stack(
        [
            jnp.sum(coords[j][:, None] * sum_cot + direction[j][:, None] * start_cot, 0)
            for j in range(2)
        ]
    )
    return first, jnp.stack(grads[::-1], 0)


def local(
    coords_inner,
    velocity,
    source,
    coords_edge,
    flux_weight,
    owner,
    local_face,
    w_first,
    b_first,
    w_hidden,
    b_hidden,
    w_last,
):
    devices = lax.axis_size(BOTH)
    inner_rows = coords_inner.shape[1]
    edge_rows = coords_edge.shape[1]
    inner_scale = 2.0 / math.sqrt(inner_rows * devices)
    face_scale = 2.0 * penalty_weight / math.sqrt(FACE_DEV * lax.axis_size("wide"))
    net = (w_first, b_first, w_hidden, b_hidden, w_last)

    _, flux, kept_edge = forward(coords_edge, flux_weight, *net)
    face = owner[:, 0] * FACE_DEV + local_face
    everyone = gather_faces(flux, face)
    all_flux = everyone[:, :4].reshape(-1)
    all_face = everyone[:, 4:].reshape(-1)

    def sums(wanted):
        return jnp.sum(
            jnp.where(wanted.astype(jnp.float32)[:, None] == all_face[None], all_flux[None], 0.0), 1
        )

    reached = sums(face)
    integral = sums(lax.axis_index("wide") * FACE_DEV + jnp.arange(FACE_DEV))

    value, slopes, kept_inner = forward(coords_inner, velocity, *net)
    inner_cot = inner_scale * (slopes + value - source)
    edge_cot = face_scale * reached

    coords = jnp.concatenate([coords_inner, coords_edge], 1)
    direction = jnp.concatenate([velocity, flux_weight], 1)
    kept = [
        tuple(None if a is None else jnp.concatenate([a, b], 0) for a, b in zip(one, two))
        for one, two in zip(kept_inner, kept_edge)
    ]
    hidden_out = jnp.concatenate([inner_cot, jnp.zeros_like(edge_cot)])[:, None]
    tangent_out = jnp.concatenate([inner_cot, edge_cot])[:, None]
    last = jnp.sum(hidden_out * kept[-1][0] + tangent_out * kept[-1][2], 0)
    first, hidden = backward(
        coords,
        direction,
        kept,
        hidden_out * w_last[None],
        tangent_out * w_last[None],
        w_first,
        w_hidden,
    )
    layers = hidden.shape[0]
    tiles = hidden.reshape(layers, 64, 8, 4, 128).transpose(0, 3, 1, 2, 4)
    small = jnp.concatenate([first.ravel(), last, jnp.zeros((512,), jnp.float32)])
    tiles, small = sum_grads(tiles.reshape(layers, TILES, 8, 128), small.reshape(2, 8, 128))
    hidden = tiles.reshape(layers, 4, 64, 8, 128).transpose(0, 2, 3, 1, 4).reshape(hidden.shape)
    small = small.ravel()
    return integral, small[:1024].reshape(2, 512), hidden, small[1024:1536]


def solution(mesh):
    points = P(None, BOTH)
    in_specs = (
        points,
        points,
        P(BOTH),
        points,
        points,
        P(BOTH, None),
        P(BOTH),
        P(),
        P(),
        P(),
        P(),
        P(),
    )
    out_specs = (P("wide"), P(), P(), P())
    return jax.shard_map(local, mesh=mesh, in_specs=in_specs, out_specs=out_specs, check_vma=False)
```
